32 devices in a mesh: gx: 4 (over x, core), gy: 2 (over y), gz: 4 (over z).
Axes of the slice: x: 2, y: 2, z: 4, core: 2. Of those that a mesh axis runs over, the one named last changes fastest.
Arguments:
- head_inputs: bfloat16 [8192, 2048], P(('gx', 'gy', 'gz')), may hold values from -6 to 6
- step_raw: float32 [8192, 32], P(('gx', 'gy', 'gz')), may hold values from -4 to 4
- state_in: bfloat16 [8192, 128], P(('gx', 'gy', 'gz')), may hold values from -0.119628906 to 0.119628906
- state_out: bfloat16 [8192, 128], P(('gx', 'gy', 'gz')), may hold values from -0.119628906 to 0.119628906
- decay_log: float32 [32], replicated, may hold values from -13.5 to -3
- step_bias: float32 [32], replicated, may hold values from -1 to 0.5
- skip_gain: float32 [32], replicated, may hold values from 0.5 to 1.5
- checkpoints: bfloat16 [32, 32, 64, 128], P(('gx', 'gy'), None, 'gz'), may hold values from -6 to 6
- out_grad: bfloat16 [8192, 2048], P(('gx', 'gy', 'gz')), may hold values from -6 to 6
Outputs:
- input_grad: bfloat16 [8192, 2048], P(('gx', 'gy', 'gz'))
- step_grad: float32 [8192, 32], P(('gx', 'gy', 'gz'))
- state_in_grad: float32 [8192, 128], P(('gx', 'gy', 'gz'))
- state_out_grad: float32 [8192, 128], P(('gx', 'gy', 'gz'))
- decay_log_grad: float32 [32], replicated
- step_bias_grad: float32 [32], replicated
- skip_gain_grad: float32 [32], replicated
The draws below stay inside these ranges and needn't reach their ends.
All inputs are finite; a program needn't handle non-finite values.
Results may differ from the reference program's by a relative error of at most 0.00065.
Values may be sent and summed in bfloat16 or wider, within the bound.
A program may use at most 128 MiB of HBM per device.

```python
import math
import jax
import jax.numpy as jnp
from jax import lax

HEADS = 32
HEAD_DIM = 64
STATE = 128
SPAN = 256
SPANS = 32
TOKENS = 8192


def draw_decay_log(key, part):
    first, second, third = jax.random.split(key, 3)
    share = 0.5
    keeping = jax.random.uniform(first, (HEADS,), jnp.float32) < share
    keep_low = max(math.log(0.5 / TOKENS), -13.5)
    keep_high = math.log(3.3 / TOKENS)
    quick_low = math.log(1.0 / (2.8 * SPAN))
    slow = jax.random.uniform(second, (HEADS,), jnp.float32, keep_low, keep_high)
    quick = jax.random.uniform(third, (HEADS,), jnp.float32, quick_low, -3.0)
    return jnp.where(keeping, slow, quick)


def levels(own_key, shape, shards, smallest, top_value):
    factor_of, own = 1.0, jax.random.fold_in(own_key, 6)
    for axis_at, shards_of in shards:
        draws = jnp.exp(jax.random.uniform(jax.random.fold_in(own, axis_at), (shards_of,), jnp.float32, smallest / len(shards), top_value / len(shards)))
        factor_of = factor_of * jnp.repeat(draws, shape[axis_at] // shards_of).reshape([-1 if axis == axis_at else 1 for axis in range(len(shape))])
    return factor_of


def bell_draw(stream_key, extent, spread, reach, cuts=(), dtype=jnp.bfloat16):
    values = jax.random.normal(stream_key, extent, jnp.float32) * spread
    if len(cuts) > 0:
        values = levels(stream_key, extent, cuts, -0.22, 0.18) * values
    return jnp.clip(values, min=-reach, max=reach).astype(dtype)


def setup_inputs(seed: int = 0) -> dict:
    keys = jax.random.split(jax.random.key(seed), 10)
    return {
        "head_inputs": bell_draw(keys[0], (TOKENS, HEADS * HEAD_DIM), 1.0, 6.0, ((0, 32),)),
        "step_raw": bell_draw(keys[1], (TOKENS, HEADS), 1.0, 4.0, ((0, 32),), jnp.float32),
        "state_in": bell_draw(keys[2], (TOKENS, STATE), 0.02, 0.119628906, ((0, 32),)),
        "state_out": bell_draw(keys[3], (TOKENS, STATE), 0.02, 0.119628906, ((0, 32),)),
        "decay_log": draw_decay_log(jax.random.fold_in(keys[9], 71), 0),
        "step_bias": jnp.clip(jax.random.uniform(keys[5], (HEADS,), jnp.float32, -1.0, 0.5), -1.0, 0.5),
        "skip_gain": jnp.clip(jax.random.uniform(keys[6], (HEADS,), jnp.float32, 0.5, 1.5), 0.5, 1.5),
        "checkpoints": bell_draw(keys[7], (SPANS, HEADS, HEAD_DIM, STATE), 1.0, 6.0, ((0, 8), (2, 4))),
        "out_grad": bell_draw(keys[8], (TOKENS, HEADS * HEAD_DIM), 1.0, 6.0, ((0, 32),)),
    }


highest = lax.Precision.HIGHEST

def block_forward(inputs, raw, b_mat, c_mat, decay_log, bias, skip, start):
    step = jax.nn.softplus(raw + bias)
    cum = jnp.cumsum(step * -jnp.exp(decay_log), axis=0)
    length = inputs.shape[0]
    rows = lax.broadcasted_iota(jnp.int32, (length, length), 0)
    cols = lax.broadcasted_iota(jnp.int32, (length, length), 1)
    lower = rows >= cols
    scores = jnp.dot(c_mat, b_mat.T, precision=highest)
    ctrans = cum.T
    gap = ctrans[:, :, None] - ctrans[:, None, :]
    mix = jnp.where(lower, jnp.exp(jnp.where(lower, gap, 0.0)), 0.0) * scores * step.T[:, None, :]
    inner = jnp.einsum('hts,shp->thp', mix, inputs, precision=highest)
    carried = jnp.einsum('tn,hpn->thp', c_mat, start, precision=highest) * jnp.exp(cum)[:, :, None]
    result = inner + carried + skip[None, :, None] * inputs
    tail = jnp.exp(cum[-1][None, :] - cum) * step
    final = jnp.exp(cum[-1])[:, None, None] * start + jnp.einsum('sh,shp,sn->hpn', tail, inputs, b_mat, precision=highest)
    return (result, final)

def span_forward(inputs, raw, b_mat, c_mat, decay_log, bias, skip, start):
    length, heads = raw.shape
    width = inputs.shape[1] // heads
    states = start.shape[2]
    block = min(8, heads)
    blocks = heads // block
    grouped = inputs.reshape(length, blocks, block, width).transpose(1, 0, 2, 3)
    raw_g = raw.reshape(length, blocks, block).transpose(1, 0, 2)

    def one_block(items):
        return block_forward(items[0], items[1], b_mat, c_mat, items[2], items[3], items[4], items[5])
    result, final = lax.map(one_block, (grouped, raw_g, decay_log.reshape(blocks, block), bias.reshape(blocks, block), skip.reshape(blocks, block), start.reshape(blocks, block, width, states)))
    result = result.transpose(1, 0, 2, 3).reshape(length, heads * width)
    return (result, final.reshape(heads, width, states))

def reference(head_inputs, step_raw, state_in, state_out, decay_log, step_bias, skip_gain, checkpoints, out_grad):
    spans = checkpoints.shape[0]
    heads = decay_log.shape[0]
    wide = head_inputs.shape[1]
    states = state_in.shape[1]
    items = (head_inputs.reshape(spans, SPAN, wide), step_raw.reshape(spans, SPAN, heads), state_in.reshape(spans, SPAN, states), state_out.reshape(spans, SPAN, states), checkpoints, out_grad.reshape(spans, SPAN, wide))

    def backward(carry, item):
        later, g_decay, g_bias, g_skip = carry
        inputs, raw, b_mat, c_mat, start, grad = item
        _, pull = jax.vjp(span_forward, inputs.astype(jnp.float32), raw, b_mat.astype(jnp.float32), c_mat.astype(jnp.float32), decay_log, step_bias, skip_gain, start.astype(jnp.float32))
        grads = pull((grad.astype(jnp.float32), later))
        new_carry = (grads[7], g_decay + grads[4], g_bias + grads[5], g_skip + grads[6])
        return (new_carry, (grads[0].astype(jnp.bfloat16), grads[1], grads[2], grads[3]))
    zeros_state = jnp.zeros(checkpoints.shape[1:], jnp.float32)
    zeros_head = jnp.zeros((heads,), jnp.float32)
    init = (zeros_state, zeros_head, zeros_head, zeros_head)
    final, outs = lax.scan(backward, init, items, reverse=True)
    input_grad = outs[0].reshape(spans * SPAN, wide)
    step_grad = outs[1].reshape(spans * SPAN, heads)
    state_in_grad = outs[2].reshape(spans * SPAN, states)
    state_out_grad = outs[3].reshape(spans * SPAN, states)
    return (input_grad, step_grad, state_in_grad, state_out_grad, final[1], final[2], final[3])
```

```python
import functools
import math

import jax
import jax.numpy as jnp
from jax import lax
from jax.experimental import pallas as pl
from jax.experimental.pallas import tpu as pltpu
from jax.sharding import PartitionSpec as P

F32, BF16 = jnp.float32, jnp.bfloat16
AXES = ("gx", "gy", "gz")
LOG2E = math.log2(math.e)
LANES = 128
NT = (((1,), (1,)), ((), ()))
TN = (((0,), (0,)), ((), ()))


def dot(a, b, dims=(((1,), (0,)), ((), ()))):
    return lax.dot_general(a, b, dims, preferred_element_type=F32)


def halves(a):
    hi = a.astype(BF16)
    return hi, (a - hi.astype(F32)).astype(BF16)


def thirds(a):
    hi = a.astype(BF16)
    rest = a - hi.astype(F32)
    mid = rest.astype(BF16)
    return hi, mid, (rest - mid.astype(F32)).astype(BF16)


def column(a, h):
    return pltpu.roll(a, lax.rem(LANES - h, LANES), 1)[:, 0:1]


def low_lanes(shape, width):
    return lax.broadcasted_iota(jnp.int32, shape, 1) < width


def pair_columns(a, j, width):
    first, second = column(a, 2 * j), column(a, 2 * j + 1)
    return jnp.where(low_lanes((a.shape[0], 2 * width), width), first, second)


def head_sum(prod, j, width):
    hi, lo = halves(prod)
    rows = lax.broadcasted_iota(jnp.int32, (4 * width, LANES), 0)
    lanes = lax.broadcasted_iota(jnp.int32, (4 * width, LANES), 1)
    head = 2 * j + jnp.where(lax.rem(rows, 2 * width) >= width, 1, 0)
    pick = jnp.where(lanes == head, 1.0, 0.0).astype(BF16)
    return dot(jnp.concatenate([hi, lo], 1), pick)


def first_kernel(
    rows, raw_ref, par_ref, g_ref, c_ref, cum_ref, dt_ref, cumt_ref, block_ref, ecum, ecumt
):
    length, heads = raw_ref.shape
    wide = g_ref.shape[1]
    width = wide // heads
    par = par_ref[...]
    z = raw_ref[...] + par[1:2, :heads]
    dt = jnp.maximum(z, 0.0) + jnp.log1p(jnp.exp(-jnp.abs(z)))
    dt_ref[...] = jnp.zeros(dt_ref.shape, F32)
    dt_ref[:, :heads] = dt
    dt = dt_ref[...]
    a = dt * -jnp.exp(par[0:1, :])
    r = lax.broadcasted_iota(jnp.int32, (length, length), 0)
    c = lax.broadcasted_iota(jnp.int32, (length, length), 1)
    lower = jnp.where(r >= c, 1.0, 0.0).astype(BF16)
    hi, mid, lo = thirds(a)
    cum = dot(lower, hi) + (dot(lower, mid) + dot(lower, lo))
    cum = cum * LOG2E
    cum_ref[...] = cum
    cumt = cum.T
    cumt_ref[...] = cumt
    ecum[...] = jnp.exp2(cum)
    ecumt[...] = jnp.exp2(cumt)
    cc = c_ref[...]
    c2 = jnp.concatenate([cc, cc], 0)
    per = 2 * width // rows

    def body(j, _):
        at = pl.ds(pl.multiple_of(j * 2 * width, 2 * width), 2 * width)
        weighted = g_ref[:, at].astype(F32) * pair_columns(ecum[...], j, width)
        hi, lo = halves(weighted)
        state = dot(jnp.concatenate([hi, lo], 0), c2, TN)
        for i in range(per):
            head = 2 * j + (i * rows) // width
            block_ref[j * per + i, 0:rows, :] = state[i * rows : (i + 1) * rows]
            decay = ecumt[pl.ds(head, 1), :][:, length - 1 : length]
            block_ref[j * per + i, rows : rows + 8, :] = jnp.broadcast_to(decay, (8, LANES))
        return 0

    lax.fori_loop(0, heads // 2, body, 0)


def scan_kernel(rows, got_ref, carry_ref):
    n = got_ref.shape[0]

    def hop(k, acc):
        at = n - 1 - k
        carry_ref[at] = acc
        part = got_ref[at]
        return part[0:rows] + part[rows : rows + 1] * acc

    lax.fori_loop(0, n, hop, jnp.zeros((rows, LANES), F32))


def inner_kernel(
    x_ref, g_ref, b_ref, c_ref, cum_ref, dt_ref, cumt_ref,
    dxi_ref, cole_ref, bg_ref, cg_ref, skip_ref, gt, dg
):
    length, wide = x_ref.shape
    heads = 2 * wide // LANES
    width = wide // heads
    half = length // 2
    r = lax.broadcasted_iota(jnp.int32, (length, length), 0)
    c = lax.broadcasted_iota(jnp.int32, (length, length), 1)
    gt[...] = jnp.where(c >= r, dot(b_ref[...], c_ref[...], NT), 0.0)
    dg[...] = jnp.zeros(dg.shape, F32)
    cole_ref[...] = jnp.zeros(cole_ref.shape, F32)
    skip_ref[...] = jnp.zeros(skip_ref.shape, F32)
    lanes = lax.broadcasted_iota(jnp.int32, (1, 2 * width), 1)
    masks_f = [jnp.where(lanes < width, 1.0, 0.0), jnp.where(lanes < width, 0.0, 1.0)]
    masks = [m.astype(BF16) for m in masks_f]

    def body(j, _):
        at = pl.ds(pl.multiple_of(j * 2 * width, 2 * width), 2 * width)
        xp, gp = x_ref[:, at], g_ref[:, at]
        gs = [gp * m for m in masks]
        overlap = jnp.sum(xp.astype(F32) * gp.astype(F32), 0, keepdims=True)
        sums = []
        parts = [[], []]
        for k in range(2):
            h = 2 * j + k
            cs, ds = column(cum_ref[...], h), column(dt_ref[...], h)
            ct = cumt_ref[pl.ds(h, 1), :]
            xk = xp * masks[k]
            skip_ref[pl.ds(h, 1), :] = overlap * masks_f[k]
            total = None
            for q in range(2):
                s0 = q * half
                rs, ts = slice(s0, s0 + half), slice(s0, length)
                dm = dot(xk[rs], gp[ts], NT)
                low = jnp.exp2(jnp.minimum(ct[:, ts] - cs[rs], 0.0))
                scores = gt[rs, ts]
                parts[q] += list(halves(low * scores))
                dl = dm * (low * ds[rs])
                dg[rs, ts] += dl
                part = jnp.sum(dl * scores, 0, keepdims=True)
                if q == 0:
                    total = part
                else:
                    total = jnp.concatenate([total[:, :half], total[:, half:] + part], 1)
            cole_ref[pl.ds(h, 1), :] = total
        for q in range(2):
            s0 = q * half
            rhs = jnp.concatenate([gs[0][s0:], gs[0][s0:], gs[1][s0:], gs[1][s0:]], 0)
            dxi_ref[s0 : s0 + half, at] = dot(jnp.concatenate(parts[q], 1), rhs)
        return 0

    lax.fori_loop(0, heads // 2, body, 0)
    d = jnp.where(c >= r, dg[...], 0.0)
    bb, cc = b_ref[...], c_ref[...]
    bg_ref[...] = dot(jnp.concatenate(halves(d), 1), jnp.concatenate([cc, cc], 0))
    cg_ref[...] = dot(jnp.concatenate(halves(d.T), 1), jnp.concatenate([bb, bb], 0))


def read_kernel(g_ref, c_ref, start_ref, cum_ref, cg_in, cg_ref, gr_ref, ecum, hi_ref, lo_ref):
    length, wide = g_ref.shape
    heads, width = start_ref.shape[0], start_ref.shape[1]
    ecum[...] = jnp.exp2(cum_ref[...])
    gr_ref[...] = jnp.zeros(gr_ref.shape, F32)
    cc = c_ref[...]

    def body(j, cg):
        at = pl.ds(pl.multiple_of(j * 2 * width, 2 * width), 2 * width)
        gp = g_ref[:, at].astype(F32)
        hp = start_ref[pl.ds(2 * j, 2)].reshape(2 * width, LANES)
        gr_ref[...] += head_sum(gp * dot(cc, hp, NT), j, width)
        hi, lo = halves(gp * pair_columns(ecum[...], j, width))
        return cg + dot(jnp.concatenate([hi, lo], 1), jnp.concatenate([hp, hp], 0))

    cg_ref[...] = lax.fori_loop(0, heads // 2, body, cg_in[...])


def last_kernel(
    x_ref, g_ref, b_ref, raw_ref, par_ref, start_ref, later_ref, cum_ref, dt_ref,
    dxi_ref, cole_ref, gr_ref, skip_ref, bg_in,
    dx_ref, draw_ref, bg_ref, part_ref, tail, ddt, ends
):
    length, wide = x_ref.shape
    heads, width = start_ref.shape[0], start_ref.shape[1]
    cum = cum_ref[...]
    tail[...] = jnp.exp2(cum[length - 1 : length] - cum)
    ddt[...] = jnp.zeros(ddt.shape, F32)
    ends[...] = jnp.zeros(ends.shape, F32)
    bb = b_ref[...]
    b2 = jnp.concatenate([bb, bb], 1)
    lanes = lax.broadcasted_iota(jnp.int32, (1, 2 * width), 1)
    masks_f = [jnp.where(lanes < width, 1.0, 0.0), jnp.where(lanes < width, 0.0, 1.0)]
    par = par_ref[...]

    def body(j, bg):
        at = pl.ds(pl.multiple_of(j * 2 * width, 2 * width), 2 * width)
        xp, gp = x_ref[:, at].astype(F32), g_ref[:, at].astype(F32)
        later = later_ref[pl.ds(2 * j, 2)].reshape(2 * width, LANES)
        hp = start_ref[pl.ds(2 * j, 2)].reshape(2 * width, LANES).astype(F32)
        lhi, llo = halves(later)
        u = dot(b2, jnp.concatenate([lhi, llo], 1), NT)
        tp, dtp = pair_columns(tail[...], j, width), pair_columns(dt_ref[...], j, width)
        skips = pair_columns(par, j, width)[2:3]
        tu = tp * u
        v = dxi_ref[:, at] + tu
        ddt[...] += head_sum(xp * v, j, width)
        dx_ref[:, at] = (dtp * v + skips * gp).astype(BF16)
        dx_w = dtp * xp
        cross = later * hp
        out = jnp.sum(dx_w * tu, 0, keepdims=True)
        for k in range(2):
            h = 2 * j + k
            own = jnp.sum(cross[k * width : (k + 1) * width], 0, keepdims=True)
            decay = jnp.exp2(column(cum_ref[length - 8 : length, :], h))[7:8]
            ends[pl.ds(h, 1), :] = own * decay + out * masks_f[k]
        whi, wlo = halves(tp * dx_w)
        return bg + dot(
            jnp.concatenate([whi, wlo, whi], 1), jnp.concatenate([lhi, lhi, llo], 0)
        )

    bg_ref[...] = lax.fori_loop(0, heads // 2, body, bg_in[...])
    dt = dt_ref[...]
    dd = ddt[...]
    dcum = cole_ref[...].T + jnp.exp2(cum) * gr_ref[...] - dt * dd
    r = lax.broadcasted_iota(jnp.int32, (length, length), 0)
    c = lax.broadcasted_iota(jnp.int32, (length, length), 1)
    upper = jnp.where(c >= r, 1.0, 0.0).astype(BF16)
    hi, mid, lo = thirds(dcum)
    da = dot(upper, hi) + (dot(upper, mid) + dot(upper, lo))
    da = da + jnp.sum(ends[...].T, 0, keepdims=True)
    rate = -jnp.exp(par[0:1])
    total = (dd + da * rate)[:, :heads]
    draw = total * jax.nn.sigmoid(raw_ref[...] + par[1:2, :heads])
    draw_ref[...] = draw
    part_ref[...] = jnp.zeros(part_ref.shape, F32)
    part_ref[0:1, :] = jnp.sum(da * dt, 0, keepdims=True) * rate
    part_ref[1:2, :heads] = jnp.sum(draw, 0, keepdims=True)
    part_ref[2:3, :] = jnp.sum(skip_ref[...].T, 0, keepdims=True)


def call(body, outs, scratch=(), flops=0, moved=0):
    return pl.pallas_call(
        body,
        out_shape=[jax.ShapeDtypeStruct(s, d) for s, d in outs],
        scratch_shapes=[pltpu.VMEM(s, F32) for s in scratch],
        compiler_params=pltpu.CompilerParams(vmem_limit_bytes=48 * 1024 * 1024),
        cost_estimate=pl.CostEstimate(flops=flops, bytes_accessed=moved, transcendentals=0),
    )


def local(n, x, raw, b_mat, c_mat, decay_log, bias, skip, checkpoints, grad):
    length, heads = raw.shape
    wide = x.shape[1]
    width = wide // heads
    states = b_mat.shape[1]
    rows = wide // n
    assert states == LANES and 2 * width == LANES and width % rows == 0
    entering = lax.all_to_all(checkpoints, "gz", split_axis=0, concat_axis=2, tiled=True)[0]
    par = jnp.pad(jnp.stack([decay_log, bias, skip]), ((0, 5), (0, LANES - heads)))
    tok = (length, LANES)
    tok_t = (LANES, length)
    cum, dt, cumt, blocks = call(
        functools.partial(first_kernel, rows),
        [(tok, F32), (tok, F32), (tok_t, F32), ((n, rows + 8, LANES), F32)],
        [tok, tok_t],
        flops=4 * length * wide * LANES,
    )(raw, par, grad, c_mat)
    got = lax.all_to_all(blocks, AXES, split_axis=0, concat_axis=0, tiled=True)
    dxi, cole, bg, cg, skips = call(
        inner_kernel,
        [((length, wide), F32), (tok_t, F32), (tok, F32), (tok, F32), ((LANES, LANES), F32)],
        [(length, length), (length, length)],
        flops=40 * length * wide * LANES,
    )(x, grad, b_mat, c_mat, cum, dt, cumt)
    (carry,) = call(
        functools.partial(scan_kernel, rows), [((n, rows, LANES), F32)]
    )(got)
    later = lax.all_to_all(carry, AXES, split_axis=0, concat_axis=0, tiled=True)
    later = later.reshape(heads, width, states)
    cg, gr = call(
        read_kernel,
        [(tok, F32), (tok, F32)],
        [tok, tok, tok],
        flops=16 * length * wide * LANES,
    )(grad, c_mat, entering, cum, cg)
    dx, draw, bg, part = call(
        last_kernel,
        [((length, wide), BF16), ((length, heads), F32), (tok, F32), ((8, LANES), F32)],
        [tok, tok, (LANES, LANES)],
        flops=16 * length * wide * LANES,
    )(x, grad, b_mat, raw, par, entering, later, cum, dt, dxi, cole, gr, skips, bg)
    total = lax.psum(part, AXES)
    return dx, draw, bg, cg, total[0, :heads], total[1, :heads], total[2, :heads]


def solution(mesh):
    tokens = P(AXES, None)
    n = math.prod(mesh.shape[a] for a in AXES)
    return jax.shard_map(
        functools.partial(local, n),
        mesh=mesh,
        in_specs=(tokens,) * 4 + (P(),) * 3 + (P(("gx", "gy"), None, "gz", None), tokens),
        out_specs=(tokens,) * 4 + (P(),) * 3,
        check_vma=False,
    )
```

```python
import functools
import math

import jax
import jax.numpy as jnp
from jax import lax
from jax.experimental import pallas as pl
from jax.experimental.pallas import tpu as pltpu
from jax.sharding import PartitionSpec as P

F32, BF16 = jnp.float32, jnp.bfloat16
AXES = ("gx", "gy", "gz")
LOG2E = math.log2(math.e)
LANES = 128
NT = (((1,), (1,)), ((), ()))
TN = (((0,), (0,)), ((), ()))


def dot(a, b, dims=(((1,), (0,)), ((), ()))):
    return lax.dot_general(a, b, dims, preferred_element_type=F32)


def halves(a):
    hi = a.astype(BF16)
    return hi, (a - hi.astype(F32)).astype(BF16)


def thirds(a):
    hi = a.astype(BF16)
    rest = a - hi.astype(F32)
    mid = rest.astype(BF16)
    return hi, mid, (rest - mid.astype(F32)).astype(BF16)


def column(a, h):
    return pltpu.roll(a, lax.rem(LANES - h, LANES), 1)[:, 0:1]


def low_lanes(shape, width):
    return lax.broadcasted_iota(jnp.int32, shape, 1) < width


def pair_columns(a, j, width):
    first, second = column(a, 2 * j), column(a, 2 * j + 1)
    return jnp.where(low_lanes((a.shape[0], 2 * width), width), first, second)


def head_sum(prod, j, width):
    hi, lo = halves(prod)
    rows = lax.broadcasted_iota(jnp.int32, (4 * width, LANES), 0)
    lanes = lax.broadcasted_iota(jnp.int32, (4 * width, LANES), 1)
    head = 2 * j + jnp.where(lax.rem(rows, 2 * width) >= width, 1, 0)
    pick = jnp.where(lanes == head, 1.0, 0.0).astype(BF16)
    return dot(jnp.concatenate([hi, lo], 1), pick)


def everything(
    n, sizes, raw_ref, par_ref, b_ref, c_ref, x_hbm, g_hbm, check_hbm,
    dx_hbm, draw_ref, bg_ref, cg_ref, sum_ref,
    x_ref, g_ref, dx_ref, start_ref, block_ref, got_ref, carry_ref, later_ref,
    cum_ref, dt_ref, ecum, tail, gr_ref, ddt, cumt_ref, ecumt, cole_ref, skip_ref, ends,
    gt, dg, dxi_ref, part_ref, parts_ref,
    load_sem, store_sem, check_send, check_recv, block_send, block_recv,
    carry_send, carry_recv, part_send, part_recv,
):
    length, heads = raw_ref.shape
    wide = x_ref.shape[1]
    width = wide // heads
    two = 2 * width
    pairs = heads // 2
    rows = wide // n
    per = two // rows
    half = length // 2
    group = sizes[2]
    zi = lax.axis_index("gz")
    me = (lax.axis_index("gx") * sizes[1] + lax.axis_index("gy")) * group + zi

    def place(d):
        return (
            lax.div(d, sizes[1] * group),
            lax.rem(lax.div(d, group), sizes[1]),
            lax.rem(d, group),
        )

    def remote(src, dst, send, recv, to):
        return pltpu.make_async_remote_copy(
            src_ref=src, dst_ref=dst, send_sem=send, recv_sem=recv,
            device_id=to, device_id_type=pl.DeviceIdType.MESH,
        )

    def other(i):
        return lax.rem(me + i, n)

    load_g = pltpu.make_async_copy(g_hbm, g_ref, load_sem.at[0])
    load_x = pltpu.make_async_copy(x_hbm, x_ref, load_sem.at[1])
    load_g.start()
    load_x.start()
    own_check = pltpu.make_async_copy(check_hbm.at[zi], start_ref.at[zi], load_sem.at[2])
    own_check.start()

    barrier = pltpu.get_barrier_semaphore()

    def greet(i, _):
        pl.semaphore_signal(
            barrier, inc=1, device_id=place(other(i)), device_id_type=pl.DeviceIdType.MESH
        )
        return 0

    lax.fori_loop(1, n, greet, 0)

    par = par_ref[...]
    dt_ref[...] = jnp.zeros(dt_ref.shape, F32)
    z = raw_ref[...] + par[1:2, :heads]
    dt_ref[:, :heads] = jnp.maximum(z, 0.0) + jnp.log1p(jnp.exp(-jnp.abs(z)))
    a = dt_ref[...] * -jnp.exp(par[0:1, :])
    r = lax.broadcasted_iota(jnp.int32, (length, length), 0)
    c = lax.broadcasted_iota(jnp.int32, (length, length), 1)
    lower = jnp.where(r >= c, 1.0, 0.0).astype(BF16)
    hi, mid, lo = thirds(a)
    cum = (dot(lower, hi) + (dot(lower, mid) + dot(lower, lo))) * LOG2E
    cum_ref[...] = cum
    cumt = cum.T
    cumt_ref[...] = cumt
    ecum[...] = jnp.exp2(cum)
    ecumt[...] = jnp.exp2(cumt)
    tail[...] = jnp.exp2(cum[length - 1 : length] - cum)
    bb, cc = b_ref[...], c_ref[...]
    gt[...] = jnp.where(c >= r, dot(bb, cc, NT), 0.0)
    dg[...] = jnp.zeros(dg.shape, F32)
    for ref in (cole_ref, skip_ref, ends, gr_ref, ddt):
        ref[...] = jnp.zeros(ref.shape, F32)
    c2 = jnp.concatenate([cc, cc], 0)
    b2 = jnp.concatenate([bb, bb], 1)
    lanes = lax.broadcasted_iota(jnp.int32, (1, two), 1)
    masks_f = [jnp.where(lanes < width, 1.0, 0.0), jnp.where(lanes < width, 0.0, 1.0)]
    masks = [m.astype(BF16) for m in masks_f]

    def columns(j):
        return pl.ds(pl.multiple_of(j * two, two), two)

    pl.semaphore_wait(barrier, n - 1)

    def check_copy(i):
        z = lax.rem(zi + i, group)
        to = (lax.axis_index("gx"), lax.axis_index("gy"), z)
        return remote(check_hbm.at[z], start_ref.at[zi], check_send, check_recv, to)

    for i in range(1, group):
        check_copy(i).start()
    load_g.wait()

    def turned(j):
        return lax.rem(j + lax.div(me, per), pairs) if per <= n else j

    def send_blocks(j):
        for i in range(per):
            d = turned(j) * per + i

            @pl.when(d != me)
            def _():
                remote(
                    block_ref.at[d], got_ref.at[me], block_send, block_recv, place(d)
                ).start()

            @pl.when(d == me)
            def _():
                pltpu.make_async_copy(block_ref.at[d], got_ref.at[me], block_recv).start()

    def first(jj, _):
        j = turned(jj)
        weighted = g_ref[:, columns(j)].astype(F32) * pair_columns(ecum[...], j, width)
        hi, lo = halves(weighted)
        state = dot(jnp.concatenate([hi, lo], 0), c2, TN)
        for i in range(per):
            head = 2 * j + (i * rows) // width
            block_ref[j * per + i, 0:rows, :] = state[i * rows : (i + 1) * rows]
            decay = ecumt[pl.ds(head, 1), :][:, length - 1 : length]
            block_ref[j * per + i, rows : rows + 8, :] = jnp.broadcast_to(decay, (8, LANES))

        @pl.when(jj > 0)
        def _():
            send_blocks(jj - 1)

        return 0

    lax.fori_loop(0, pairs, first, 0)
    load_x.wait()
    send_blocks(pairs - 1)

    def inner(j, _):
        at = columns(j)
        xp, gp = x_ref[:, at], g_ref[:, at]
        gs = [gp * m for m in masks]
        overlap = jnp.sum(xp.astype(F32) * gp.astype(F32), 0, keepdims=True)
        parts = [[], []]
        for k in range(2):
            h = 2 * j + k
            cs, ds = column(cum_ref[...], h), column(dt_ref[...], h)
            ct = cumt_ref[pl.ds(h, 1), :]
            xk = xp * masks[k]
            skip_ref[pl.ds(h, 1), :] = overlap * masks_f[k]
            total = None
            for q in range(2):
                s0 = q * half
                rs, ts = slice(s0, s0 + half), slice(s0, length)
                dm = dot(xk[rs], gp[ts], NT)
                low = jnp.exp2(jnp.minimum(ct[:, ts] - cs[rs], 0.0))
                scores = gt[rs, ts]
                parts[q] += list(halves(low * scores))
                dl = dm * (low * ds[rs])
                dg[rs, ts] += dl
                part = jnp.sum(dl * scores, 0, keepdims=True)
                if q == 0:
                    total = part
                else:
                    total = jnp.concatenate([total[:, :half], total[:, half:] + part], 1)
            cole_ref[pl.ds(h, 1), :] = total
        for q in range(2):
            s0 = q * half
            rhs = jnp.concatenate([gs[0][s0:], gs[0][s0:], gs[1][s0:], gs[1][s0:]], 0)
            dxi_ref[s0 : s0 + half, at] = dot(jnp.concatenate(parts[q], 1), rhs)
        return 0

    lax.fori_loop(0, pairs, inner, 0)

    pltpu.make_async_copy(got_ref, got_ref, block_recv).wait()

    def hop(k, acc):
        at = n - 1 - k
        carry_ref[at] = acc
        part = got_ref[at]
        return part[0:rows] + part[rows : rows + 1] * acc

    lax.fori_loop(0, n, hop, jnp.zeros((rows, LANES), F32))
    mine = lax.div(me, per)

    def send_carry(i, _):
        d = other(i)
        remote(
            carry_ref.at[d], later_ref.at[me], carry_send, carry_recv.at[mine], place(d)
        ).start()
        return 0

    lax.fori_loop(1, n, send_carry, 0)
    pltpu.make_async_copy(carry_ref.at[me], later_ref.at[me], carry_recv.at[mine]).start()

    d = jnp.where(c >= r, dg[...], 0.0)
    bg_ref[...] = dot(jnp.concatenate(halves(d), 1), jnp.concatenate([cc, cc], 0))
    cg_ref[...] = dot(jnp.concatenate(halves(d.T), 1), jnp.concatenate([bb, bb], 0))

    own_check.wait()
    for i in range(1, group):
        check_copy(i).wait_send()
    arrived = start_ref.at[pl.ds(0, group - 1)]
    pltpu.make_async_copy(arrived, arrived, check_recv).wait()

    def entering(j):
        return jnp.concatenate(
            [start_ref[q, 2 * j + k] for k in range(2) for q in range(group)], 0
        )

    def read(j, cg):
        gp = g_ref[:, columns(j)].astype(F32)
        hp = entering(j)
        gr_ref[...] += head_sum(gp * dot(cc, hp, NT), j, width)
        hi, lo = halves(gp * pair_columns(ecum[...], j, width))
        return cg + dot(jnp.concatenate([hi, lo], 1), jnp.concatenate([hp, hp], 0))

    cg_ref[...] = lax.fori_loop(0, pairs, read, cg_ref[...])

    def last(jj, bg):
        j = lax.rem(mine + pairs - jj, pairs)
        at = columns(j)
        come = later_ref.at[pl.ds(j * per, per)]
        pltpu.make_async_copy(come, come, carry_recv.at[j]).wait()
        later = jnp.concatenate([later_ref[j * per + i] for i in range(per)], 0)
        xp, gp = x_ref[:, at].astype(F32), g_ref[:, at].astype(F32)
        hp = entering(j).astype(F32)
        lhi, llo = halves(later)
        u = dot(b2, jnp.concatenate([lhi, llo], 1), NT)
        tp, dtp = pair_columns(tail[...], j, width), pair_columns(dt_ref[...], j, width)
        skips = pair_columns(par_ref[...], j, width)[2:3]
        tu = tp * u
        v = dxi_ref[:, at] + tu
        ddt[...] += head_sum(xp * v, j, width)
        dx_ref[:, at] = (dtp * v + skips * gp).astype(BF16)
        dx_w = dtp * xp
        cross = later * hp
        out = jnp.sum(dx_w * tu, 0, keepdims=True)
        for k in range(2):
            h = 2 * j + k
            own = jnp.sum(cross[k * width : (k + 1) * width], 0, keepdims=True)
            decay = ecumt[pl.ds(h, 1), :][:, length - 1 : length]
            ends[pl.ds(h, 1), :] = own * decay + out * masks_f[k]
        whi, wlo = halves(tp * dx_w)
        return bg + dot(
            jnp.concatenate([whi, wlo, whi], 1), jnp.concatenate([lhi, lhi, llo], 0)
        )

    bg = lax.fori_loop(0, pairs, last, bg_ref[...])
    dt = dt_ref[...]
    dd = ddt[...]
    dcum = cole_ref[...].T + ecum[...] * gr_ref[...] - dt * dd
    upper = jnp.where(c >= r, 1.0, 0.0).astype(BF16)
    hi, mid, lo = thirds(dcum)
    da = dot(upper, hi) + (dot(upper, mid) + dot(upper, lo))
    da = da + jnp.sum(ends[...].T, 0, keepdims=True)
    rate = -jnp.exp(par[0:1])
    total = (dd + da * rate)[:, :heads]
    draw = total * jax.nn.sigmoid(raw_ref[...] + par[1:2, :heads])
    part_ref[...] = jnp.zeros(part_ref.shape, F32)
    part_ref[0:1, :] = jnp.sum(da * dt, 0, keepdims=True) * rate
    part_ref[1:2, :heads] = jnp.sum(draw, 0, keepdims=True)
    part_ref[2:3, :] = jnp.sum(skip_ref[...].T, 0, keepdims=True)
    store = pltpu.make_async_copy(dx_ref, dx_hbm, store_sem)
    store.start()
    draw_ref[...] = draw
    bg_ref[...] = bg

    def send_part(i, _):
        remote(part_ref, parts_ref.at[me], part_send, part_recv, place(other(i))).start()
        return 0

    lax.fori_loop(1, n, send_part, 0)
    pltpu.make_async_copy(part_ref, parts_ref.at[me], part_recv).start()
    sent = block_ref.at[pl.ds(0, n - 1)]
    pltpu.make_async_copy(sent, sent, block_send).wait()
    sent = carry_ref.at[pl.ds(0, n - 1)]
    pltpu.make_async_copy(sent, sent, carry_send).wait()
    pltpu.make_async_copy(parts_ref, parts_ref, part_recv).wait()
    sum_ref[...] = lax.fori_loop(
        0, n, lambda i, acc: acc + parts_ref[i], jnp.zeros(sum_ref.shape, F32)
    )
    sent = parts_ref.at[pl.ds(0, n - 1)]
    pltpu.make_async_copy(sent, sent, part_send).wait()
    store.wait()


def local(sizes, x, raw, b_mat, c_mat, decay_log, bias, skip, checkpoints, grad):
    n = math.prod(sizes)
    length, heads = raw.shape
    wide = x.shape[1]
    width = wide // heads
    rows = wide // n
    assert b_mat.shape[1] == LANES and 2 * width == LANES and width % rows == 0
    assert heads <= LANES and sizes[2] == checkpoints.shape[0]
    par = jnp.pad(jnp.stack([decay_log, bias, skip]), ((0, 5), (0, LANES - heads)))
    tok, tok_t, square = (length, LANES), (LANES, length), (LANES, LANES)
    pairs = heads // 2
    vmem = [
        ((length, wide), BF16), ((length, wide), BF16), ((length, wide), BF16),
        (checkpoints.shape, BF16),
        ((n, rows + 8, LANES), F32), ((n, rows + 8, LANES), F32),
        ((n, rows, LANES), F32), ((n, rows, LANES), F32),
        (tok, F32), (tok, F32), (tok, F32), (tok, F32), (tok, F32), (tok, F32),
        (tok_t, F32), (tok_t, F32), (tok_t, F32), (square, F32), (square, F32),
        ((length, length), F32), ((length, length), F32), ((length, wide), F32),
        ((8, LANES), F32), ((n, 8, LANES), F32),
    ]
    dma = pltpu.SemaphoreType.DMA
    near = pl.BlockSpec(memory_space=pltpu.VMEM)
    far = pl.BlockSpec(memory_space=pltpu.HBM)
    outs = [
        ((length, wide), BF16), ((length, heads), F32), (tok, F32), (tok, F32),
        ((8, LANES), F32),
    ]
    dx, draw, bg, cg, total = pl.pallas_call(
        functools.partial(everything, n, sizes),
        out_shape=[jax.ShapeDtypeStruct(s, d) for s, d in outs],
        in_specs=[near] * 4 + [far] * 3,
        out_specs=[far] + [near] * 4,
        scratch_shapes=[pltpu.VMEM(s, d) for s, d in vmem]
        + [dma((3,)), dma(()), dma(()), dma(()), dma(()), dma(()), dma(()), dma((pairs,)),
           dma(()), dma(())],
        compiler_params=pltpu.CompilerParams(
            collective_id=0, has_side_effects=True, vmem_limit_bytes=56 * 1024 * 1024
        ),
        cost_estimate=pl.CostEstimate(
            flops=80 * length * wide * LANES, bytes_accessed=4 * length * wide, transcendentals=0
        ),
    )(raw, par, b_mat, c_mat, x, grad, checkpoints)
    return dx, draw, bg, cg, total[0, :heads], total[1, :heads], total[2, :heads]


def solution(mesh):
    tokens = P(AXES, None)
    sizes = tuple(mesh.shape[a] for a in AXES)
    return jax.shard_map(
        functools.partial(local, sizes),
        mesh=mesh,
        in_specs=(tokens,) * 4 + (P(),) * 3 + (P(("gx", "gy"), None, "gz", None), tokens),
        out_specs=(tokens,) * 4 + (P(),) * 3,
        check_vma=False,
    )
```

```python
import functools
import math

import jax
import jax.numpy as jnp
from jax import lax
from jax.experimental import pallas as pl
from jax.experimental.pallas import tpu as pltpu
from jax.sharding import PartitionSpec as P

F32, BF16 = jnp.float32, jnp.bfloat16
AXES = ("gx", "gy", "gz")
LOG2E = math.log2(math.e)
LANES = 128
NT = (((1,), (1,)), ((), ()))
TN = (((0,), (0,)), ((), ()))


def dot(a, b, dims=(((1,), (0,)), ((), ()))):
    return lax.dot_general(a, b, dims, preferred_element_type=F32)


def halves(a):
    hi = a.astype(BF16)
    return hi, (a - hi.astype(F32)).astype(BF16)


def thirds(a):
    hi = a.astype(BF16)
    rest = a - hi.astype(F32)
    mid = rest.astype(BF16)
    return hi, mid, (rest - mid.astype(F32)).astype(BF16)


def column(a, h):
    return pltpu.roll(a, lax.rem(LANES - h, LANES), 1)[:, 0:1]


def low_lanes(shape, width):
    return lax.broadcasted_iota(jnp.int32, shape, 1) < width


def pair_columns(a, j, width):
    first, second = column(a, 2 * j), column(a, 2 * j + 1)
    return jnp.where(low_lanes((a.shape[0], 2 * width), width), first, second)


def head_sum(prod, j, width):
    hi, lo = halves(prod)
    rows = lax.broadcasted_iota(jnp.int32, (4 * width, LANES), 0)
    lanes = lax.broadcasted_iota(jnp.int32, (4 * width, LANES), 1)
    head = 2 * j + jnp.where(lax.rem(rows, 2 * width) >= width, 1, 0)
    pick = jnp.where(lanes == head, 1.0, 0.0).astype(BF16)
    return dot(jnp.concatenate([hi, lo], 1), pick)


def everything(
    n, sizes, rawt_ref, decay_ref, bias_ref, gain_ref, b_ref, c_ref, x_hbm, g_hbm, check_hbm,
    dx_hbm, drawt_ref, bg_ref, cg_ref, sum_ref,
    x_ref, g_ref, dx_ref, start_ref, block_ref, got_ref, carry_ref, later_ref,
    cum_ref, dt_ref, ecum, tail, gr_ref, ddt, cumt_ref, ecumt, cole_ref, skip_ref, ends,
    gt, dg, dxi_ref, part_ref, parts_ref, par_ref, row_ref, rows_ref, rates_ref,
    load_sem, store_sem, row_send, row_recv, check_send, check_recv, block_send, block_recv,
    carry_send, carry_recv, part_send, part_recv,
):
    heads, length = rawt_ref.shape
    wide = x_ref.shape[1]
    width = wide // heads
    two = 2 * width
    pairs = heads // 2
    rows = wide // n
    per = two // rows
    half = length // 2
    group = sizes[2]
    zi = lax.axis_index("gz")
    me = (lax.axis_index("gx") * sizes[1] + lax.axis_index("gy")) * group + zi

    def place(d):
        return (
            lax.div(d, sizes[1] * group),
            lax.rem(lax.div(d, group), sizes[1]),
            lax.rem(d, group),
        )

    def remote(src, dst, send, recv, to):
        return pltpu.make_async_remote_copy(
            src_ref=src, dst_ref=dst, send_sem=send, recv_sem=recv,
            device_id=to, device_id_type=pl.DeviceIdType.MESH,
        )

    def other(i):
        return lax.rem(me + i, n)

    load_g = pltpu.make_async_copy(g_hbm, g_ref, load_sem.at[0])
    load_x = pltpu.make_async_copy(x_hbm, x_ref, load_sem.at[1])
    load_g.start()
    load_x.start()
    own_check = pltpu.make_async_copy(check_hbm.at[zi], start_ref.at[zi], load_sem.at[2])
    own_check.start()

    barrier = pltpu.get_barrier_semaphore()

    def greet(i, _):
        pl.semaphore_signal(
            barrier, inc=1, device_id=place(other(i)), device_id_type=pl.DeviceIdType.MESH
        )
        return 0

    lax.fori_loop(1, n, greet, 0)

    par_ref[...] = jnp.zeros(par_ref.shape, F32)
    for at, ref in enumerate((decay_ref, bias_ref, gain_ref)):
        par_ref[at : at + 1, :heads] = ref[...]
    par = par_ref[...]
    cumt_ref[...] = jnp.zeros(cumt_ref.shape, F32)
    cumt_ref[:heads, :] = rawt_ref[...]
    z = cumt_ref[...].T + par[1:2]
    dt_ref[...] = jnp.maximum(z, 0.0) + jnp.log1p(jnp.exp(-jnp.abs(z)))
    a = dt_ref[...] * -jnp.exp(par[0:1, :])
    r = lax.broadcasted_iota(jnp.int32, (length, length), 0)
    c = lax.broadcasted_iota(jnp.int32, (length, length), 1)
    lower = jnp.where(r >= c, 1.0, 0.0).astype(BF16)
    hi, mid, lo = thirds(a)
    cum = (dot(lower, hi) + (dot(lower, mid) + dot(lower, lo))) * LOG2E
    cum_ref[...] = cum
    cumt = cum.T
    cumt_ref[...] = cumt
    ecum[...] = jnp.exp2(cum)
    row_ref[...] = jnp.exp2(cum[length - 1 : length])
    ecumt[...] = jnp.exp2(cumt)
    tail[...] = jnp.exp2(cum[length - 1 : length] - cum)
    bb, cc = b_ref[...], c_ref[...]
    gt[...] = jnp.where(c >= r, dot(bb, cc, NT), 0.0)
    dg[...] = jnp.zeros(dg.shape, F32)
    for ref in (cole_ref, skip_ref, ends, gr_ref, ddt):
        ref[...] = jnp.zeros(ref.shape, F32)
    c2 = jnp.concatenate([cc, cc], 0)
    b2 = jnp.concatenate([bb, bb], 1)
    lanes = lax.broadcasted_iota(jnp.int32, (1, two), 1)
    masks_f = [jnp.where(lanes < width, 1.0, 0.0), jnp.where(lanes < width, 0.0, 1.0)]
    masks = [m.astype(BF16) for m in masks_f]

    def columns(j):
        return pl.ds(pl.multiple_of(j * two, two), two)

    pl.semaphore_wait(barrier, n - 1)

    def check_copy(i):
        z = lax.rem(zi + i, group)
        to = (lax.axis_index("gx"), lax.axis_index("gy"), z)
        return remote(check_hbm.at[z], start_ref.at[zi], check_send, check_recv, to)

    load_g.wait()

    def send_row(i, _):
        remote(row_ref, rows_ref.at[me], row_send, row_recv, place(other(i))).start()
        return 0

    lax.fori_loop(1, n, send_row, 0)
    pltpu.make_async_copy(row_ref, rows_ref.at[me], row_recv).start()

    def turned(j):
        return lax.rem(j + lax.div(me, per), pairs) if per <= n else j

    def send_blocks(j):
        for i in range(per):
            d = turned(j) * per + i

            @pl.when(d != me)
            def _():
                remote(
                    block_ref.at[d], got_ref.at[me], block_send, block_recv, place(d)
                ).start()

            @pl.when(d == me)
            def _():
                pltpu.make_async_copy(block_ref.at[d], got_ref.at[me], block_recv).start()

    def first(jj, _):
        j = turned(jj)
        weighted = g_ref[:, columns(j)].astype(F32) * pair_columns(ecum[...], j, width)
        hi, lo = halves(weighted)
        state = dot(jnp.concatenate([hi, lo], 0), c2, TN)
        for i in range(per):
            block_ref[j * per + i] = state[i * rows : (i + 1) * rows]

        @pl.when(jj > 0)
        def _():
            send_blocks(jj - 1)

        return 0

    lax.fori_loop(0, pairs, first, 0)
    load_x.wait()
    send_blocks(pairs - 1)
    for i in range(1, group):
        check_copy(i).start()

    def inner(j, _):
        at = columns(j)
        xp, gp = x_ref[:, at], g_ref[:, at]
        gs = [gp * m for m in masks]
        overlap = jnp.sum(xp.astype(F32) * gp.astype(F32), 0, keepdims=True)
        parts = [[], []]
        for k in range(2):
            h = 2 * j + k
            cs, ds = column(cum_ref[...], h), column(dt_ref[...], h)
            ct = cumt_ref[pl.ds(h, 1), :]
            xk = xp * masks[k]
            skip_ref[pl.ds(h, 1), :] = overlap * masks_f[k]
            total = None
            for q in range(2):
                s0 = q * half
                rs, ts = slice(s0, s0 + half), slice(s0, length)
                dm = dot(xk[rs], gp[ts], NT)
                low = jnp.exp2(jnp.minimum(ct[:, ts] - cs[rs], 0.0))
                scores = gt[rs, ts]
                parts[q] += list(halves(low * scores))
                dl = dm * (low * ds[rs])
                dg[rs, ts] += dl
                part = jnp.sum(dl * scores, 0, keepdims=True)
                if q == 0:
                    total = part
                else:
                    total = jnp.concatenate([total[:, :half], total[:, half:] + part], 1)
            cole_ref[pl.ds(h, 1), :] = total
        for q in range(2):
            s0 = q * half
            rhs = jnp.concatenate([gs[0][s0:], gs[0][s0:], gs[1][s0:], gs[1][s0:]], 0)
            dxi_ref[s0 : s0 + half, at] = dot(jnp.concatenate(parts[q], 1), rhs)
        return 0

    lax.fori_loop(0, pairs, inner, 0)

    pltpu.make_async_copy(rows_ref, rows_ref, row_recv).wait()
    head = lax.div(me * rows, width)
    pick = jnp.where(lax.broadcasted_iota(jnp.int32, (1, LANES), 1) == head, 1.0, 0.0)

    def rate_of(i, _):
        rate = jnp.sum(rows_ref[i] * pick, 1, keepdims=True)
        rates_ref[i] = jnp.broadcast_to(rate, (1, LANES))
        return 0

    lax.fori_loop(0, n, rate_of, 0)
    pltpu.make_async_copy(got_ref, got_ref, block_recv).wait()

    def hop(k, acc):
        at = n - 1 - k
        carry_ref[at] = acc
        return got_ref[at] + rates_ref[at] * acc

    lax.fori_loop(0, n, hop, jnp.zeros((rows, LANES), F32))
    mine = lax.div(me, per)

    def send_carry(i, _):
        d = other(i)
        remote(
            carry_ref.at[d], later_ref.at[me], carry_send, carry_recv.at[mine], place(d)
        ).start()
        return 0

    lax.fori_loop(1, n, send_carry, 0)
    pltpu.make_async_copy(carry_ref.at[me], later_ref.at[me], carry_recv.at[mine]).start()

    d = jnp.where(c >= r, dg[...], 0.0)
    bg_ref[...] = dot(jnp.concatenate(halves(d), 1), jnp.concatenate([cc, cc], 0))
    cg_ref[...] = dot(jnp.concatenate(halves(d.T), 1), jnp.concatenate([bb, bb], 0))

    own_check.wait()
    for i in range(1, group):
        check_copy(i).wait_send()
    arrived = start_ref.at[pl.ds(0, group - 1)]
    pltpu.make_async_copy(arrived, arrived, check_recv).wait()

    def entering(j):
        return jnp.concatenate(
            [start_ref[q, 2 * j + k] for k in range(2) for q in range(group)], 0
        )

    def read(j, cg):
        gp = g_ref[:, columns(j)].astype(F32)
        hp = entering(j)
        gr_ref[...] += head_sum(gp * dot(cc, hp, NT), j, width)
        hi, lo = halves(gp * pair_columns(ecum[...], j, width))
        return cg + dot(jnp.concatenate([hi, lo], 1), jnp.concatenate([hp, hp], 0))

    cg_ref[...] = lax.fori_loop(0, pairs, read, cg_ref[...])

    def last(jj, bg):
        j = lax.rem(mine + pairs - jj, pairs)
        at = columns(j)
        come = later_ref.at[pl.ds(j * per, per)]
        pltpu.make_async_copy(come, come, carry_recv.at[j]).wait()
        later = jnp.concatenate([later_ref[j * per + i] for i in range(per)], 0)
        xp, gp = x_ref[:, at].astype(F32), g_ref[:, at].astype(F32)
        hp = entering(j).astype(F32)
        lhi, llo = halves(later)
        u = dot(b2, jnp.concatenate([lhi, llo], 1), NT)
        tp, dtp = pair_columns(tail[...], j, width), pair_columns(dt_ref[...], j, width)
        skips = pair_columns(par_ref[...], j, width)[2:3]
        tu = tp * u
        v = dxi_ref[:, at] + tu
        ddt[...] += head_sum(xp * v, j, width)
        dx_ref[:, at] = (dtp * v + skips * gp).astype(BF16)
        dx_w = dtp * xp
        cross = later * hp
        out = jnp.sum(dx_w * tu, 0, keepdims=True)
        for k in range(2):
            h = 2 * j + k
            own = jnp.sum(cross[k * width : (k + 1) * width], 0, keepdims=True)
            decay = ecumt[pl.ds(h, 1), :][:, length - 1 : length]
            ends[pl.ds(h, 1), :] = own * decay + out * masks_f[k]
        whi, wlo = halves(tp * dx_w)
        return bg + dot(
            jnp.concatenate([whi, wlo, whi], 1), jnp.concatenate([lhi, lhi, llo], 0)
        )

    bg = lax.fori_loop(0, pairs, last, bg_ref[...])
    store = pltpu.make_async_copy(dx_ref, dx_hbm, store_sem)
    store.start()
    dt = dt_ref[...]
    dd = ddt[...]
    dcum = cole_ref[...].T + ecum[...] * gr_ref[...] - dt * dd
    upper = jnp.where(c >= r, 1.0, 0.0).astype(BF16)
    hi, mid, lo = thirds(dcum)
    da = dot(upper, hi) + (dot(upper, mid) + dot(upper, lo))
    da = da + jnp.sum(ends[...].T, 0, keepdims=True)
    rate = -jnp.exp(par[0:1])
    cumt_ref[:heads, :] = rawt_ref[...]
    draw = (dd + da * rate) * jax.nn.sigmoid(cumt_ref[...].T + par[1:2])
    part_ref[...] = jnp.zeros(part_ref.shape, F32)
    part_ref[0:1, :] = jnp.sum(da * dt, 0, keepdims=True) * rate
    part_ref[1:2, :] = jnp.sum(draw, 0, keepdims=True)
    part_ref[2:3, :] = jnp.sum(skip_ref[...].T, 0, keepdims=True)
    drawt_ref[...] = draw.T[:heads]
    bg_ref[...] = bg

    def send_part(i, _):
        remote(part_ref, parts_ref.at[me], part_send, part_recv, place(other(i))).start()
        return 0

    lax.fori_loop(1, n, send_part, 0)
    pltpu.make_async_copy(part_ref, parts_ref.at[me], part_recv).start()
    sent = block_ref.at[pl.ds(0, n - 1)]
    pltpu.make_async_copy(sent, sent, block_send).wait()
    sent = carry_ref.at[pl.ds(0, n - 1)]
    pltpu.make_async_copy(sent, sent, carry_send).wait()
    pltpu.make_async_copy(parts_ref, parts_ref, part_recv).wait()
    sum_ref[...] = lax.fori_loop(
        0, n, lambda i, acc: acc + parts_ref[i], jnp.zeros(sum_ref.shape, F32)
    )
    sent = parts_ref.at[pl.ds(0, n - 1)]
    pltpu.make_async_copy(sent, sent, part_send).wait()
    sent = rows_ref.at[pl.ds(0, n - 1)]
    pltpu.make_async_copy(sent, sent, row_send).wait()
    store.wait()


def local(sizes, x, raw, b_mat, c_mat, decay_log, bias, skip, checkpoints, grad):
    n = math.prod(sizes)
    length, heads = raw.shape
    wide = x.shape[1]
    width = wide // heads
    rows = wide // n
    assert b_mat.shape[1] == LANES and 2 * width == LANES and width % rows == 0
    assert heads <= LANES and sizes[2] == checkpoints.shape[0]
    tok, tok_t, square = (length, LANES), (LANES, length), (LANES, LANES)
    pairs = heads // 2
    vmem = [
        ((length, wide), BF16), ((length, wide), BF16), ((length, wide), BF16),
        (checkpoints.shape, BF16),
        ((n, rows, LANES), F32), ((n, rows, LANES), F32),
        ((n, rows, LANES), F32), ((n, rows, LANES), F32),
        (tok, F32), (tok, F32), (tok, F32), (tok, F32), (tok, F32), (tok, F32),
        (tok_t, F32), (tok_t, F32), (tok_t, F32), (square, F32), (square, F32),
        ((length, length), F32), ((length, length), F32), ((length, wide), F32),
        ((8, LANES), F32), ((n, 8, LANES), F32), ((8, LANES), F32),
        ((1, LANES), F32), ((n, 1, LANES), F32), ((n, 1, LANES), F32),
    ]
    dma = pltpu.SemaphoreType.DMA
    near = pl.BlockSpec(memory_space=pltpu.VMEM)
    far = pl.BlockSpec(memory_space=pltpu.HBM)
    outs = [
        ((length, wide), BF16), ((heads, length), F32), (tok, F32), (tok, F32),
        ((8, LANES), F32),
    ]
    dx, draw, bg, cg, total = pl.pallas_call(
        functools.partial(everything, n, sizes),
        out_shape=[jax.ShapeDtypeStruct(s, d) for s, d in outs],
        in_specs=[near] * 6 + [far] * 3,
        out_specs=[far] + [near] * 4,
        scratch_shapes=[pltpu.VMEM(s, d) for s, d in vmem]
        + [dma((3,)), dma(()), dma(()), dma(()), dma(()), dma(()), dma(()), dma(()), dma(()), dma((pairs,)),
           dma(()), dma(())],
        compiler_params=pltpu.CompilerParams(
            collective_id=0, has_side_effects=True, vmem_limit_bytes=56 * 1024 * 1024
        ),
        cost_estimate=pl.CostEstimate(
            flops=80 * length * wide * LANES, bytes_accessed=4 * length * wide, transcendentals=0
        ),
    )(raw.T, decay_log[None], bias[None], skip[None], b_mat, c_mat, x, grad, checkpoints)
    return dx, draw.T, bg, cg, total[0, :heads], total[1, :heads], total[2, :heads]


def solution(mesh):
    tokens = P(AXES, None)
    sizes = tuple(mesh.shape[a] for a in AXES)
    return jax.shard_map(
        functools.partial(local, sizes),
        mesh=mesh,
        in_specs=(tokens,) * 4 + (P(),) * 3 + (P(("gx", "gy"), None, "gz", None), tokens),
        out_specs=(tokens,) * 4 + (P(),) * 3,
        check_vma=False,
    )
```

```python
import functools
import math

import jax
import jax.numpy as jnp
from jax import lax
from jax.experimental import pallas as pl
from jax.experimental.pallas import tpu as pltpu
from jax.sharding import PartitionSpec as P

F32, BF16 = jnp.float32, jnp.bfloat16
AXES = ("gx", "gy", "gz")
LOG2E = math.log2(math.e)
LANES = 128
NT = (((1,), (1,)), ((), ()))
TN = (((0,), (0,)), ((), ()))


def dot(a, b, dims=(((1,), (0,)), ((), ()))):
    return lax.dot_general(a, b, dims, preferred_element_type=F32)


def halves(a):
    hi = a.astype(BF16)
    return hi, (a - hi.astype(F32)).astype(BF16)


def thirds(a):
    hi = a.astype(BF16)
    rest = a - hi.astype(F32)
    mid = rest.astype(BF16)
    return hi, mid, (rest - mid.astype(F32)).astype(BF16)


def column(a, h):
    return pltpu.roll(a, lax.rem(LANES - h, LANES), 1)[:, 0:1]


def low_lanes(shape, width):
    return lax.broadcasted_iota(jnp.int32, shape, 1) < width


def pair_columns(a, j, width):
    first, second = column(a, 2 * j), column(a, 2 * j + 1)
    return jnp.where(low_lanes((a.shape[0], 2 * width), width), first, second)


def head_sum(prod, j, width):
    hi, lo = halves(prod)
    rows = lax.broadcasted_iota(jnp.int32, (4 * width, LANES), 0)
    lanes = lax.broadcasted_iota(jnp.int32, (4 * width, LANES), 1)
    head = 2 * j + jnp.where(lax.rem(rows, 2 * width) >= width, 1, 0)
    pick = jnp.where(lanes == head, 1.0, 0.0).astype(BF16)
    return dot(jnp.concatenate([hi, lo], 1), pick)


def everything(
    n, sizes, rawt_ref, decay_ref, bias_ref, gain_ref, b_ref, c_ref, x_hbm, g_hbm, check_hbm,
    dx_hbm, drawt_ref, bg_ref, cg_ref, sum_ref,
    x_ref, g_ref, dx_ref, start_ref, block_ref, got_ref, carry_ref, later_ref,
    cum_ref, dt_ref, ecum, tail, gr_ref, ddt, cumt_ref, ecumt, cole_ref, skip_ref, ends,
    gt, dg, dxi_ref, part_ref, parts_ref, par_ref, row_ref, rows_ref, rates_ref,
    load_sem, store_sem, row_send, row_recv, check_send, check_recv, block_send, block_recv,
    carry_send, carry_recv, part_send, part_recv,
):
    heads, length = rawt_ref.shape
    wide = x_ref.shape[1]
    width = wide // heads
    two = 2 * width
    pairs = heads // 2
    rows = wide // n
    per = two // rows
    half = length // 2
    group = sizes[2]
    zi = lax.axis_index("gz")
    me = (lax.axis_index("gx") * sizes[1] + lax.axis_index("gy")) * group + zi

    def place(d):
        return (
            lax.div(d, sizes[1] * group),
            lax.rem(lax.div(d, group), sizes[1]),
            lax.rem(d, group),
        )

    def remote(src, dst, send, recv, to):
        return pltpu.make_async_remote_copy(
            src_ref=src, dst_ref=dst, send_sem=send, recv_sem=recv,
            device_id=to, device_id_type=pl.DeviceIdType.MESH,
        )

    def other(i):
        return lax.rem(me + i, n)

    load_g = pltpu.make_async_copy(g_hbm, g_ref, load_sem.at[0])
    load_x = pltpu.make_async_copy(x_hbm, x_ref, load_sem.at[1])
    load_g.start()
    load_x.start()
    own_check = pltpu.make_async_copy(check_hbm.at[zi], start_ref.at[zi], load_sem.at[2])
    own_check.start()

    barrier = pltpu.get_barrier_semaphore()

    def greet(i, _):
        pl.semaphore_signal(
            barrier, inc=1, device_id=place(other(i)), device_id_type=pl.DeviceIdType.MESH
        )
        return 0

    lax.fori_loop(1, n, greet, 0)

    par_ref[...] = jnp.zeros(par_ref.shape, F32)
    for at, ref in enumerate((decay_ref, bias_ref, gain_ref)):
        par_ref[at : at + 1, :heads] = ref[...]
    par = par_ref[...]
    cumt_ref[...] = jnp.zeros(cumt_ref.shape, F32)
    cumt_ref[:heads, :] = rawt_ref[...]
    z = cumt_ref[...].T + par[1:2]
    dt_ref[...] = jnp.maximum(z, 0.0) + jnp.log1p(jnp.exp(-jnp.abs(z)))
    a = dt_ref[...] * -jnp.exp(par[0:1, :])
    r = lax.broadcasted_iota(jnp.int32, (length, length), 0)
    c = lax.broadcasted_iota(jnp.int32, (length, length), 1)
    lower = jnp.where(r >= c, 1.0, 0.0).astype(BF16)
    hi, mid, lo = thirds(a)
    cum = (dot(lower, hi) + (dot(lower, mid) + dot(lower, lo))) * LOG2E
    cum_ref[...] = cum
    cumt = cum.T
    cumt_ref[...] = cumt
    ecum[...] = jnp.exp2(cum)
    row_ref[...] = jnp.exp2(cum[length - 1 : length])
    ecumt[...] = jnp.exp2(cumt)
    tail[...] = jnp.exp2(cum[length - 1 : length] - cum)
    bb, cc = b_ref[...], c_ref[...]
    gt[...] = jnp.where(c >= r, dot(bb, cc, NT), 0.0)
    dg[...] = jnp.zeros(dg.shape, F32)
    for ref in (cole_ref, skip_ref, ends, gr_ref, ddt):
        ref[...] = jnp.zeros(ref.shape, F32)
    c2 = jnp.concatenate([cc, cc], 0)
    b2 = jnp.concatenate([bb, bb], 1)
    lanes = lax.broadcasted_iota(jnp.int32, (1, two), 1)
    masks_f = [jnp.where(lanes < width, 1.0, 0.0), jnp.where(lanes < width, 0.0, 1.0)]
    masks = [m.astype(BF16) for m in masks_f]

    def columns(j):
        return pl.ds(pl.multiple_of(j * two, two), two)

    pl.semaphore_wait(barrier, n - 1)

    def check_copy(i):
        z = lax.rem(zi + i, group)
        to = (lax.axis_index("gx"), lax.axis_index("gy"), z)
        return remote(check_hbm.at[z], start_ref.at[zi], check_send, check_recv, to)

    load_g.wait()

    def send_row(i, _):
        remote(row_ref, rows_ref.at[me], row_send, row_recv, place(other(i))).start()
        return 0

    lax.fori_loop(1, n, send_row, 0)
    pltpu.make_async_copy(row_ref, rows_ref.at[me], row_recv).start()

    def turned(j):
        return lax.rem(j + lax.div(me, per), pairs) if per <= n else j

    def send_blocks(j):
        for i in range(per):
            d = turned(j) * per + i

            @pl.when(d != me)
            def _():
                remote(
                    block_ref.at[d], got_ref.at[me], block_send, block_recv, place(d)
                ).start()

            @pl.when(d == me)
            def _():
                pltpu.make_async_copy(block_ref.at[d], got_ref.at[me], block_recv).start()

    def first(jj, _):
        j = turned(jj)
        weighted = g_ref[:, columns(j)].astype(F32) * pair_columns(ecum[...], j, width)
        hi, lo = halves(weighted)
        state = dot(jnp.concatenate([hi, lo], 0), c2, TN)
        for i in range(per):
            block_ref[j * per + i] = state[i * rows : (i + 1) * rows]

        @pl.when(jj > 0)
        def _():
            send_blocks(jj - 1)

        return 0

    lax.fori_loop(0, pairs, first, 0)
    load_x.wait()
    send_blocks(pairs - 1)
    for i in range(1, group):
        check_copy(i).start()

    def inner(j, _):
        at = columns(j)
        xp, gp = x_ref[:, at], g_ref[:, at]
        gs = [gp * m for m in masks]
        overlap = jnp.sum(xp.astype(F32) * gp.astype(F32), 0, keepdims=True)
        parts = [[], []]
        for k in range(2):
            h = 2 * j + k
            cs, ds = column(cum_ref[...], h), column(dt_ref[...], h)
            ct = cumt_ref[pl.ds(h, 1), :]
            xk = xp * masks[k]
            skip_ref[pl.ds(h, 1), :] = overlap * masks_f[k]
            total = None
            for q in range(2):
                s0 = q * half
                rs, ts = slice(s0, s0 + half), slice(s0, length)
                dm = dot(xk[rs], gp[ts], NT)
                low = jnp.exp2(jnp.minimum(ct[:, ts] - cs[rs], 0.0))
                scores = gt[rs, ts]
                parts[q] += list(halves(low * scores))
                dl = dm * (low * ds[rs])
                dg[rs, ts] += dl
                part = jnp.sum(dl * scores, 0, keepdims=True)
                if q == 0:
                    total = part
                else:
                    total = jnp.concatenate([total[:, :half], total[:, half:] + part], 1)
            cole_ref[pl.ds(h, 1), :] = total
        for q in range(2):
            s0 = q * half
            rhs = jnp.concatenate([gs[0][s0:], gs[0][s0:], gs[1][s0:], gs[1][s0:]], 0)
            dxi_ref[s0 : s0 + half, at] = dot(jnp.concatenate(parts[q], 1), rhs)
        return 0

    lax.fori_loop(0, pairs, inner, 0)

    pltpu.make_async_copy(rows_ref, rows_ref, row_recv).wait()
    head = lax.div(me * rows, width)
    pick = jnp.where(lax.broadcasted_iota(jnp.int32, (1, LANES), 1) == head, 1.0, 0.0)

    def rate_of(i, _):
        rate = jnp.sum(rows_ref[i] * pick, 1, keepdims=True)
        rates_ref[i] = jnp.broadcast_to(rate, (1, LANES))
        return 0

    lax.fori_loop(0, n, rate_of, 0)
    pltpu.make_async_copy(got_ref, got_ref, block_recv).wait()

    def hop(k, acc):
        at = n - 1 - k
        carry_ref[at] = acc
        return got_ref[at] + rates_ref[at] * acc

    lax.fori_loop(0, n, hop, jnp.zeros((rows, LANES), F32))
    mine = lax.div(me, per)

    def send_carry(i, _):
        d = other(i)
        remote(
            carry_ref.at[d], later_ref.at[me], carry_send, carry_recv.at[mine], place(d)
        ).start()
        return 0

    lax.fori_loop(1, n, send_carry, 0)
    pltpu.make_async_copy(carry_ref.at[me], later_ref.at[me], carry_recv.at[mine]).start()

    d = jnp.where(c >= r, dg[...], 0.0)
    bg_ref[...] = dot(jnp.concatenate(halves(d), 1), jnp.concatenate([cc, cc], 0))
    cg_ref[...] = dot(jnp.concatenate(halves(d.T), 1), jnp.concatenate([bb, bb], 0))

    own_check.wait()
    for i in range(1, group):
        check_copy(i).wait_send()
    arrived = start_ref.at[pl.ds(0, group - 1)]
    pltpu.make_async_copy(arrived, arrived, check_recv).wait()

    def entering(j):
        return jnp.concatenate(
            [start_ref[q, 2 * j + k] for k in range(2) for q in range(group)], 0
        )

    def read(j, cg):
        gp = g_ref[:, columns(j)].astype(F32)
        hp = entering(j)
        gr_ref[...] += head_sum(gp * dot(cc, hp, NT), j, width)
        hi, lo = halves(gp * pair_columns(ecum[...], j, width))
        return cg + dot(jnp.concatenate([hi, lo], 1), jnp.concatenate([hp, hp], 0))

    cg_ref[...] = lax.fori_loop(0, pairs, read, cg_ref[...])

    def last(jj, bg):
        j = lax.rem(mine + pairs - jj, pairs)
        at = columns(j)
        come = later_ref.at[pl.ds(j * per, per)]
        pltpu.make_async_copy(come, come, carry_recv.at[j]).wait()
        later = jnp.concatenate([later_ref[j * per + i] for i in range(per)], 0)
        xp, gp = x_ref[:, at].astype(F32), g_ref[:, at].astype(F32)
        hp = entering(j).astype(F32)
        lhi, llo = halves(later)
        u = dot(b2, jnp.concatenate([lhi, llo], 1), NT)
        tp, dtp = pair_columns(tail[...], j, width), pair_columns(dt_ref[...], j, width)
        skips = pair_columns(par_ref[...], j, width)[2:3]
        tu = tp * u
        v = dxi_ref[:, at] + tu
        ddt[...] += head_sum(xp * v, j, width)
        dx_ref[:, at] = (dtp * v + skips * gp).astype(BF16)
        dx_w = dtp * xp
        cross = later * hp
        out = jnp.sum(dx_w * tu, 0, keepdims=True)
        for k in range(2):
            h = 2 * j + k
            own = jnp.sum(cross[k * width : (k + 1) * width], 0, keepdims=True)
            decay = ecumt[pl.ds(h, 1), :][:, length - 1 : length]
            ends[pl.ds(h, 1), :] = own * decay + out * masks_f[k]
        whi, wlo = halves(tp * dx_w)
        return bg + dot(
            jnp.concatenate([whi, wlo, whi], 1), jnp.concatenate([lhi, lhi, llo], 0)
        )

    bg = lax.fori_loop(0, pairs, last, bg_ref[...])
    store = pltpu.make_async_copy(dx_ref, dx_hbm, store_sem)
    store.start()
    dt = dt_ref[...]
    dd = ddt[...]
    dcum = cole_ref[...].T + ecum[...] * gr_ref[...] - dt * dd
    upper = jnp.where(c >= r, 1.0, 0.0).astype(BF16)
    hi, mid, lo = thirds(dcum)
    da = dot(upper, hi) + (dot(upper, mid) + dot(upper, lo))
    da = da + jnp.sum(ends[...].T, 0, keepdims=True)
    rate = -jnp.exp(par[0:1])
    cumt_ref[:heads, :] = rawt_ref[...]
    draw = (dd + da * rate) * jax.nn.sigmoid(cumt_ref[...].T + par[1:2])
    part_ref[...] = jnp.zeros(part_ref.shape, F32)
    part_ref[0:1, :] = jnp.sum(da * dt, 0, keepdims=True) * rate
    part_ref[1:2, :] = jnp.sum(draw, 0, keepdims=True)
    part_ref[2:3, :] = jnp.sum(skip_ref[...].T, 0, keepdims=True)
    drawt_ref[...] = draw.T[:heads]
    bg_ref[...] = bg

    def send_part(i, _):
        remote(part_ref, parts_ref.at[me], part_send, part_recv, place(other(i))).start()
        return 0

    lax.fori_loop(1, n, send_part, 0)
    pltpu.make_async_copy(part_ref, parts_ref.at[me], part_recv).start()
    sent = block_ref.at[pl.ds(0, n - 1)]
    pltpu.make_async_copy(sent, sent, block_send).wait()
    sent = carry_ref.at[pl.ds(0, n - 1)]
    pltpu.make_async_copy(sent, sent, carry_send).wait()
    pltpu.make_async_copy(parts_ref, parts_ref, part_recv).wait()
    sum_ref[...] = lax.fori_loop(
        0, n, lambda i, acc: acc + parts_ref[i], jnp.zeros(sum_ref.shape, F32)
    )
    sent = parts_ref.at[pl.ds(0, n - 1)]
    pltpu.make_async_copy(sent, sent, part_send).wait()
    sent = rows_ref.at[pl.ds(0, n - 1)]
    pltpu.make_async_copy(sent, sent, row_send).wait()
    store.wait()


def hand_over(
    dx_in, draw_in, bg_in, cg_in, sum_in, dx_ref, draw_ref, bg_ref, cg_ref, *sum_refs
):
    dx_ref[...] = dx_in[...]

    @pl.when(pl.program_id(0) == 0)
    def _():
        draw_ref[...] = draw_in[...]
        bg_ref[...] = bg_in[...]
        cg_ref[...] = cg_in[...]
        for at, ref in enumerate(sum_refs):
            ref[...] = sum_in[at : at + 1, : ref.shape[1]]


def local(sizes, x, raw, b_mat, c_mat, decay_log, bias, skip, checkpoints, grad):
    n = math.prod(sizes)
    length, heads = raw.shape
    wide = x.shape[1]
    width = wide // heads
    rows = wide // n
    assert b_mat.shape[1] == LANES and 2 * width == LANES and width % rows == 0
    assert heads <= LANES and sizes[2] == checkpoints.shape[0]
    tok, tok_t, square = (length, LANES), (LANES, length), (LANES, LANES)
    pairs = heads // 2
    vmem = [
        ((length, wide), BF16), ((length, wide), BF16), ((length, wide), BF16),
        (checkpoints.shape, BF16),
        ((n, rows, LANES), F32), ((n, rows, LANES), F32),
        ((n, rows, LANES), F32), ((n, rows, LANES), F32),
        (tok, F32), (tok, F32), (tok, F32), (tok, F32), (tok, F32), (tok, F32),
        (tok_t, F32), (tok_t, F32), (tok_t, F32), (square, F32), (square, F32),
        ((length, length), F32), ((length, length), F32), ((length, wide), F32),
        ((8, LANES), F32), ((n, 8, LANES), F32), ((8, LANES), F32),
        ((1, LANES), F32), ((n, 1, LANES), F32), ((n, 1, LANES), F32),
    ]
    dma = pltpu.SemaphoreType.DMA
    near = pl.BlockSpec(memory_space=pltpu.VMEM)
    far = pl.BlockSpec(memory_space=pltpu.HBM)
    outs = [
        ((length, wide), BF16), ((heads, length), F32), (tok, F32), (tok, F32),
        ((8, LANES), F32),
    ]
    dx, draw, bg, cg, total = pl.pallas_call(
        functools.partial(everything, n, sizes),
        out_shape=[jax.ShapeDtypeStruct(s, d) for s, d in outs],
        in_specs=[near] * 6 + [far] * 3,
        out_specs=[far] + [near] * 4,
        scratch_shapes=[pltpu.VMEM(s, d) for s, d in vmem]
        + [dma((3,)), dma(()), dma(()), dma(()), dma(()), dma(()), dma(()), dma(()), dma(()), dma((pairs,)),
           dma(()), dma(())],
        compiler_params=pltpu.CompilerParams(
            collective_id=0, has_side_effects=True, vmem_limit_bytes=56 * 1024 * 1024
        ),
        cost_estimate=pl.CostEstimate(
            flops=80 * length * wide * LANES, bytes_accessed=4 * length * wide, transcendentals=0
        ),
    )(raw.T, decay_log[None], bias[None], skip[None], b_mat, c_mat, x, grad, checkpoints)
    steps = 4

    def whole(shape):
        return pl.BlockSpec(shape, lambda i: (0, 0))

    moved = pl.BlockSpec((length // steps, wide), lambda i: (i, 0))
    small = [whole((heads, length)), whole(tok), whole(tok)]
    one = (1, heads)
    dx, draw, bg, cg, *sums = pl.pallas_call(
        hand_over,
        grid=(steps,),
        out_shape=[jax.ShapeDtypeStruct(s, d) for s, d in outs[:4] + [(one, F32)] * 3],
        in_specs=[moved] + small + [whole((8, LANES))],
        out_specs=[moved] + small + [whole(one)] * 3,
        compiler_params=pltpu.CompilerParams(vmem_limit_bytes=56 * 1024 * 1024),
    )(dx, draw, bg, cg, total)
    return (dx, draw.T, bg, cg, *(part[0] for part in sums))


def solution(mesh):
    tokens = P(AXES, None)
    sizes = tuple(mesh.shape[a] for a in AXES)
    return jax.shard_map(
        functools.partial(local, sizes),
        mesh=mesh,
        in_specs=(tokens,) * 4 + (P(),) * 3 + (P(("gx", "gy"), None, "gz", None), tokens),
        out_specs=(tokens,) * 4 + (P(),) * 3,
        check_vma=False,
    )
```
